256 devices in a mesh: side: 2 (over core), group: 16 (over y, z_lo), head: 8 (over x, z_hi).
Axes of the slice: x: 4, y: 4, z: 8 (z_hi: 2, z_lo: 4; z = z_hi * 4 + z_lo), core: 2. Of those that a mesh axis runs over, the one named last changes fastest.
Arguments:
- pool_rows: bfloat16 [2, 6144, 4096], P('side', ('group', 'head')), may hold values from -24 to 24
- pool_weight: bfloat16 [2, 4096, 8192], P('side', 'group', 'head'), as said below
- lengths: int32 [16, 3], replicated, may hold values from 1 to 192, 384 in all within a row
- owner: int32 [16, 3], replicated, may hold values from 0 to 15, as said below
Outputs:
- pool_out: bfloat16 [2, 6144, 4096], P('side', 'group', 'head')
The draws below stay inside these ranges and needn't reach their ends.
Inputs may be any that keep to these rules, and one draw needn't show every extreme that they name: owner[p, j] is p with the binary digits of m_j flipped, where m_j = owner[0, j] is the same for every p; the m_j differ between slots, and every binary digit below 16 is set in some m_j. So the 3 requests of a prefill group go to different decode groups, and every decode group receives exactly one request for each slot j. `lengths`: each row sums to 384. `pool_weight`: independent normal entries of deviation 1 / sqrt(4096).
All inputs are finite; a program needn't handle non-finite values.
Results may differ from the reference program's by a relative error of at most 0.0061.
Values may be sent and summed in bfloat16 or wider, within the bound.
No kernel may reach another device: no remote copies, remote signals or barrier semaphores. Data moves between devices by JAX's collectives and lax.ppermute only.
A program may use at most 128 MiB of HBM per device.

```python
import math
import jax
import jax.numpy as jnp
import numpy as np
from jax import lax

D = 4096
HEADS = 16
HEAD_DIM = 256
ROWS_DEV = 48
REQ_G = 3
MEM_G = 384
MAXLEN = 192
TOK = 6144
N_GROUP = 16
N_HEAD = 8


def weight_table(key):
    return jax.random.normal(jax.random.fold_in(key, 41), (2, D, 2 * D), jnp.float32) * D ** (-0.5)


def draw_pool_weight(key, part):
    return weight_table(key).astype(jnp.bfloat16)


def draw_pool_rows(key, part):
    noise = jnp.clip(jax.random.normal(jax.random.fold_in(key, 7), (2, TOK, D), jnp.float32), -6.0, 6.0)
    return noise.astype(jnp.bfloat16)


def draw_owner(key, part):
    half = N_GROUP // 2
    other = jax.random.randint(jax.random.fold_in(key, 17), (1,), 0, N_GROUP - 2).astype(jnp.int32)
    other = jnp.where(other >= half, other + 1, other).astype(jnp.int32)
    fixed = jnp.array([half, N_GROUP - 1], jnp.int32)
    flips = jnp.concatenate([fixed, other], axis=0)[:REQ_G]
    order = jax.random.permutation(jax.random.fold_in(key, 29), REQ_G)
    flips = flips[order].astype(jnp.int32)
    groups = jnp.arange(N_GROUP, dtype=jnp.int32)
    return jnp.bitwise_xor(groups[:, None], flips[None, :]).astype(jnp.int32)


def profile(amount, total, reach, slope):
    portions = [(1 << 20) // math.isqrt(grade ** slope) + 1 for grade in range(2, amount + 1)]
    rest, counts = total - reach - (amount - 1), [1] * (amount - 1)
    while rest > 0:
        candidates = [i for i in range(amount - 1) if counts[i] < reach]
        whole, budget = sum([portions[i] for i in candidates]), rest
        for i in candidates:
            extra = min(reach - counts[i], max(1, budget * portions[i] // whole), rest)
            counts[i] = counts[i] + extra
            rest = rest - extra
    return np.array([reach] + counts)


def uneven(key, count, total, reach, lean):
    if count == 2:
        one = jax.random.randint(key, (), max(1, total - reach), min(reach, total - 1) + 1)
        return jnp.stack([one, total - one])
    tallies = jnp.asarray(profile(count, total, reach, lean), jnp.int32)
    twos = (count - 1) // 2
    source_of, receiver = tallies[1:1 + 2 * twos:2], tallies[2:2 + 2 * twos:2]
    slack = jnp.minimum(source_of - 1, reach - receiver)
    moved = jax.random.randint(jax.random.fold_in(key, 1), (twos,), 0, 1 << 20) % (slack + 1)
    tallies = tallies.at[1:1 + 2 * twos:2].set(source_of - moved).at[2:2 + 2 * twos:2].set(receiver + moved)
    return tallies[jax.random.permutation(jax.random.fold_in(key, 2), count)]


def setup_inputs(seed: int = 0) -> dict:
    arg_keys = jax.random.split(jax.random.key(seed), 5)
    pool_rows = draw_pool_rows(jax.random.fold_in(arg_keys[4], 71), 0)
    pool_weight = draw_pool_weight(jax.random.fold_in(arg_keys[4], 71), 0)
    lengths = jax.vmap(lambda own: uneven(own, REQ_G, MEM_G, MAXLEN, 2))(jax.random.split(arg_keys[2], N_GROUP)).reshape((N_GROUP, REQ_G)).astype(jnp.int32)
    owner = draw_owner(jax.random.fold_in(arg_keys[4], 71), 0)
    return dict(pool_rows=pool_rows, pool_weight=pool_weight, lengths=lengths, owner=owner)


def reference(pool_rows, pool_weight, lengths, owner):
    mem_g = ROWS_DEV * N_HEAD
    wide = D // N_HEAD
    q_req = mem_g // REQ_G
    maxlen = mem_g // 2
    scale = 1.0 / (HEAD_DIM ** 0.5)

    def halves(index):
        proj = jnp.dot(pool_rows[index], pool_weight[index], preferred_element_type=jnp.float32)
        proj = proj.reshape(TOK, N_HEAD, 2, wide)
        return proj[:, :, 0, :].reshape(TOK, D), proj[:, :, 1, :].reshape(TOK, D)

    first, second = halves(0)
    keys = first.astype(jnp.bfloat16)
    values = second.astype(jnp.bfloat16)
    queries = halves(1)[0].astype(jnp.bfloat16)
    out_weight = pool_weight[1].reshape(D, N_HEAD, 2, wide)[:, :, 1, :].reshape(D, D)
    starts = jnp.cumsum(lengths, axis=1).astype(jnp.int32) - lengths
    padding = jnp.zeros((maxlen, D), jnp.bfloat16)
    keys_pad = jnp.concatenate([keys, padding], axis=0)
    values_pad = jnp.concatenate([values, padding], axis=0)
    groups = jnp.arange(N_GROUP, dtype=jnp.int32)

    def one_group(decode):
        pieces = []
        for slot in range(REQ_G):
            hit = owner[:, slot] == decode
            source = jnp.sum(jnp.where(hit, groups, 0)).astype(jnp.int32)
            begin = jnp.sum(jnp.where(hit, starts[:, slot], 0)).astype(jnp.int32)
            count = jnp.sum(jnp.where(hit, lengths[:, slot], 0)).astype(jnp.int32)
            first_row = (source * mem_g + begin).astype(jnp.int32)
            key_rows = lax.dynamic_slice_in_dim(keys_pad, first_row, maxlen, 0).reshape(maxlen, HEADS, HEAD_DIM)
            value_rows = lax.dynamic_slice_in_dim(values_pad, first_row, maxlen, 0).reshape(maxlen, HEADS, HEAD_DIM)
            query_start = (decode * mem_g + slot * q_req).astype(jnp.int32)
            query_rows = lax.dynamic_slice_in_dim(queries, query_start, q_req, 0).reshape(q_req, HEADS, HEAD_DIM)
            scores = jnp.einsum("qeh,keh->eqk", query_rows.astype(jnp.float32), key_rows.astype(jnp.float32)) * scale
            valid = jnp.arange(maxlen, dtype=jnp.int32) < count
            scores = jnp.where(valid[None, None, :], scores, -1e30)
            peak = jnp.max(scores, axis=-1, keepdims=True)
            expo = jnp.where(valid[None, None, :], jnp.exp(scores - peak), 0.0)
            total = jnp.sum(expo, axis=-1)
            probs = expo.astype(jnp.bfloat16)
            mixed = jnp.einsum("eqk,keh->eqh", probs.astype(jnp.float32), value_rows.astype(jnp.float32))
            mixed = mixed / total[:, :, None]
            pieces.append(jnp.transpose(mixed, (1, 0, 2)).reshape(q_req, D))
        return jnp.concatenate(pieces, axis=0).astype(jnp.bfloat16)

    attended = lax.map(one_group, groups).reshape(TOK, D)
    decoded = lax.dot_general(attended, out_weight, (((1,), (1,)), ((), ())), preferred_element_type=jnp.float32)
    return jnp.stack([keys, decoded.astype(jnp.bfloat16)], axis=0)
```

```python
import jax
import jax.numpy as jnp
from jax import lax
from jax.sharding import Mesh
from jax.sharding import PartitionSpec as P

HEAD_DIM = 256
AXES = ("side", "y", "zl", "x", "zh")


def ring(value, axis, by):
    count = lax.axis_size(axis)
    return lax.ppermute(value, axis, [(i, (i + by) % count) for i in range(count)])


def ring_swap(value, bit):
    return lax.ppermute(value, "zl", [(i, i ^ bit) for i in range(4)])


def ring_gather(block, axis):
    half = block.shape[0] // 2
    left = ring(block, axis, 1)
    right = ring(block, axis, -1)
    far_a = ring(left[:half], axis, 1)
    far_b = ring(right[half:], axis, -1)
    return [block, left, right, jnp.concatenate([far_a, far_b], axis=0)]


def exchange(blocks, flips, source):
    groups = lax.axis_size("y") * lax.axis_size("zl")
    count = flips.shape[0]
    size = blocks.shape[0] // count

    def route(flip):
        pairs = [(source * groups + p, (1 - source) * groups + (p ^ flip)) for p in range(groups)]
        return lambda b: lax.ppermute(b, ("side", "y", "zl"), pairs)

    def step(j, held):
        block = lax.dynamic_slice(blocks, (j * size, 0), (size, blocks.shape[1]))
        moved = lax.switch(flips[j], [route(flip) for flip in range(groups)], block)
        return lax.dynamic_update_slice(held, moved, (j * size, 0))

    return lax.fori_loop(0, count, step, jnp.zeros_like(blocks))


def on_device(pool_rows, pool_weight, lengths, owner):
    side = lax.axis_index("side")
    y, zl, x, zh = (lax.axis_index(a) for a in AXES[1:])
    ny = lax.axis_size("y")
    requests = lengths.shape[1]
    w = pool_weight[0]
    depth, width = w.shape
    wide = width // 2
    scale = 1.0 / HEAD_DIM**0.5

    u1 = ring_swap(w, 1)
    u2 = ring_swap(w, 2)
    u3 = ring_swap(u2, 1)
    slots = [zl, zl ^ 1, zl ^ 2, zl ^ 3]
    places = [y, (y - 1) % ny, (y + 1) % ny, (y + 2) % ny]
    units = [ring_gather(u, "y") for u in (w, u1, u2, u3)]

    mine = pool_rows[0]
    other = lax.ppermute(mine, "zh", [(0, 1), (1, 0)])
    pair = jnp.concatenate([jnp.where(zh == 0, mine, other), jnp.where(zh == 0, other, mine)], axis=0)
    parts = ring_gather(pair, "x")
    span = pair.shape[0]
    rows = jnp.zeros((4 * span, mine.shape[1]), jnp.bfloat16)
    for part, place in zip(parts, [x, (x - 1) % 4, (x + 1) % 4, (x + 2) % 4]):
        rows = lax.dynamic_update_slice(rows, part, (place * span, 0))
    mem_g = rows.shape[0]
    q_req = mem_g // requests

    acc = jnp.zeros((mem_g, width), jnp.float32)
    tail = jnp.zeros((ny * 4 * depth, wide), jnp.bfloat16)
    for k in range(4):
        for d in range(4):
            at = (places[d] * 4 + slots[k]) * depth
            cols = lax.dynamic_slice(rows, (0, at), (mem_g, depth))
            acc = acc + jnp.dot(cols, units[k][d], preferred_element_type=jnp.float32)
            tail = lax.dynamic_update_slice(tail, units[k][d][:, wide:], (at, 0))
    first = acc[:, :wide].astype(jnp.bfloat16)
    second = acc[:, wide:].astype(jnp.bfloat16)

    flips = owner[0]
    asked = exchange(first, flips, 1)
    group = y * 4 + zl
    counts = lax.dynamic_index_in_dim(lengths, group, 0, keepdims=False)
    ends = jnp.cumsum(counts)
    begin = jnp.repeat(ends - counts, q_req)[:, None]
    end = jnp.repeat(ends, q_req)[:, None]
    at = jnp.arange(mem_g, dtype=jnp.int32)[None, :]
    valid = (at >= begin) & (at < end)
    outs = []
    for e in range(wide // HEAD_DIM):
        part = slice(e * HEAD_DIM, (e + 1) * HEAD_DIM)
        scores = lax.dot_general(
            asked[:, part], first[:, part], (((1,), (1,)), ((), ())), preferred_element_type=jnp.float32
        )
        scores = jnp.where(valid, scores * scale, -1e30)
        peak = jnp.max(scores, axis=-1, keepdims=True)
        expo = jnp.where(valid, jnp.exp(scores - peak), 0.0)
        total = jnp.sum(expo, axis=-1, keepdims=True)
        mixed = jnp.dot(expo.astype(jnp.bfloat16), second[:, part], preferred_element_type=jnp.float32)
        outs.append((mixed / total).astype(jnp.bfloat16))
    answer = jnp.concatenate(outs, axis=1)
    attended = exchange(answer, flips, 0)

    def project(to):
        weight = lax.dynamic_slice(tail, (to * (2 * wide), 0), (2 * wide, wide))
        return lax.dot_general(
            attended, weight, (((1,), (1,)), ((), ())), preferred_element_type=jnp.float32
        )

    def send(by):
        pairs = [(4 + i, 4 + (i + by) % 4) for i in range(4)]
        return lax.ppermute(project((x + by) % 4).astype(jnp.bfloat16), ("side", "x"), pairs)

    got = [send(by) for by in (2, 1, 3)]
    partial = project(x)
    for g in got:
        partial = partial + g.astype(jnp.float32)
    keep = lax.dynamic_slice(partial, (0, zh * wide), (mem_g, wide))
    give = lax.dynamic_slice(partial, (0, (1 - zh) * wide), (mem_g, wide)).astype(jnp.bfloat16)
    taken = lax.ppermute(give, ("side", "zh"), [(2, 3), (3, 2)])
    decoded = (keep + taken.astype(jnp.float32)).astype(jnp.bfloat16)
    return jnp.where(side == 0, first, decoded)[None]


def solution(mesh):
    torus = Mesh(mesh.devices.reshape(mesh.shape["side"], 4, 4, 4, 2), AXES)
    in_specs = (
        P("side", ("y", "zl", "x", "zh"), None),
        P("side", ("y", "zl"), ("x", "zh")),
        P(),
        P(),
    )
    out_specs = P("side", ("y", "zl"), ("x", "zh"))
    return jax.shard_map(on_device, mesh=torus, in_specs=in_specs, out_specs=out_specs, check_vma=False)
```

```python
import jax
import jax.numpy as jnp
from jax import lax
from jax.sharding import Mesh
from jax.sharding import PartitionSpec as P


HEAD_DIM = 256
AXES = ("side", "y", "zl", "x", "zh")


def ring(value, axis, by):
    count = lax.axis_size(axis)
    return lax.ppermute(value, axis, [(i, (i + by) % count) for i in range(count)])


def ring_swap(value, bit):
    return lax.ppermute(value, "zl", [(i, i ^ bit) for i in range(4)])


def after(value, *done):
    return lax.optimization_barrier((value, *done))[0]


def exchange(block, flip):
    groups = lax.axis_size("y") * lax.axis_size("zl")

    def route(by):
        pairs = [(p, groups + (p ^ by)) for p in range(groups)]
        return lambda b: lax.ppermute(b, ("side", "y", "zl"), pairs)

    return lax.switch(flip, [route(by) for by in range(groups)], block)


def attend(queries, memory, count, wide):
    maxlen = memory.shape[0]
    valid = (jnp.arange(maxlen, dtype=jnp.int32) < count)[None, :]
    scale = 1.0 / HEAD_DIM**0.5
    outs = []
    for e in range(wide // HEAD_DIM):
        keys = memory[:, e * HEAD_DIM : (e + 1) * HEAD_DIM]
        values = memory[:, wide + e * HEAD_DIM : wide + (e + 1) * HEAD_DIM]
        scores = lax.dot_general(
            queries[:, e * HEAD_DIM : (e + 1) * HEAD_DIM],
            keys,
            (((1,), (1,)), ((), ())),
            preferred_element_type=jnp.float32,
        )
        scores = jnp.where(valid, scores * scale, -1e30)
        peak = jnp.max(scores, axis=-1, keepdims=True)
        expo = jnp.where(valid, jnp.exp(scores - peak), 0.0)
        total = jnp.sum(expo, axis=-1, keepdims=True)
        mixed = jnp.dot(expo.astype(jnp.bfloat16), values, preferred_element_type=jnp.float32)
        outs.append((mixed / total).astype(jnp.bfloat16))
    return jnp.concatenate(outs, axis=1)


def body(pool_rows, pool_weight, lengths, owner):
    side = lax.axis_index("side")
    y, zl, x, zh = (lax.axis_index(a) for a in AXES[1:])
    ny = lax.axis_size("y")
    requests = lengths.shape[1]
    w = pool_weight[0]
    mine = pool_rows[0]
    depth, width = w.shape
    wide = width // 2
    half = depth // 2
    count, model = mine.shape

    p0, m0 = ring(w, "y", 1), ring(w, "y", -1)
    u1, u2 = ring_swap(w, 1), ring_swap(w, 2)
    other = lax.ppermute(mine, "zh", [(0, 1), (1, 0)])
    a0, b0 = ring(p0[:half], "y", 1), ring(m0[half:], "y", -1)
    p1, m1 = ring(u1, "y", 1), ring(u1, "y", -1)
    a1, b1 = ring(p1[:half], "y", 1), ring(m1[half:], "y", -1)
    other = after(other, p1, m1)
    pair = jnp.concatenate([jnp.where(zh == 0, mine, other), jnp.where(zh == 0, other, mine)], axis=0)
    px, mx = ring(pair, "x", 1), ring(pair, "x", -1)
    u2 = after(u2, pair)
    u3 = ring_swap(u2, 1)
    p2, m2 = ring(u2, "y", 1), ring(u2, "y", -1)
    u3 = after(u3, a1, b1)
    p3, m3 = ring(u3, "y", 1), ring(u3, "y", -1)
    p2, m2 = after(p2, u3), after(m2, u3)
    a2, b2 = ring(p2[:half], "y", 1), ring(m2[half:], "y", -1)
    px, mx = after(px, p2, m2), after(mx, p2, m2)
    ax, bx = ring(px[:count], "x", 1), ring(mx[count:], "x", -1)
    p3, m3 = after(p3, px, mx), after(m3, px, mx)
    a3, b3 = ring(p3[:half], "y", 1), ring(m3[half:], "y", -1)

    rows = jnp.zeros((8 * count, model), jnp.bfloat16)
    fx = jnp.concatenate([ax, bx], axis=0)
    for part, place in zip((pair, px, mx, fx), (x, (x - 1) % 4, (x + 1) % 4, (x + 2) % 4)):
        rows = lax.dynamic_update_slice(rows, part, (place * 2 * count, 0))
    mem_g = rows.shape[0]
    q_req = mem_g // requests
    maxlen = mem_g // 2

    acc = jnp.zeros((mem_g, width), jnp.float32)
    tail = jnp.zeros((ny * 4 * depth, wide), jnp.bfloat16)
    places = [y, (y - 1) % ny, (y + 1) % ny, (y + 2) % ny]
    near = [(w, p0, m0, a0, b0), (u1, p1, m1, a1, b1), (u2, p2, m2, a2, b2), (u3, p3, m3, a3, b3)]
    for k, (u, p, m, a, b) in enumerate(near):
        far = jnp.concatenate([a, b], axis=0)
        for block, place in zip((u, p, m, far), places):
            at = (place * 4 + (zl ^ k)) * depth
            cols = lax.dynamic_slice(rows, (0, at), (mem_g, depth))
            acc = acc + jnp.dot(cols, block, preferred_element_type=jnp.float32)
            tail = lax.dynamic_update_slice(tail, block[:, wide:], (at, 0))
    cached = acc.astype(jnp.bfloat16)
    first = cached[:, :wide]

    group = y * 4 + zl
    flips = owner[0]
    own = lax.dynamic_index_in_dim(lengths, group, 0, keepdims=False)
    begins = jnp.cumsum(own) - own
    padded = jnp.concatenate([cached, jnp.zeros((maxlen, width), jnp.bfloat16)], axis=0)
    blocks = [lax.dynamic_slice(padded, (begins[j], 0), (maxlen, width)) for j in range(requests)]

    def serve(j, memory):
        length = lax.dynamic_slice(lengths, (group ^ flips[j], j), (1, 1))[0, 0]
        return attend(first[j * q_req : (j + 1) * q_req], memory, length, wide)

    def project(attended, to):
        weight = lax.dynamic_slice(tail, (to * (2 * wide), 0), (2 * wide, wide))
        return lax.dot_general(
            attended, weight, (((1,), (1,)), ((), ())), preferred_element_type=jnp.float32
        )

    def along_x(attended):
        got = []
        for by in (2, 1, 3):
            pairs = [(4 + i, 4 + (i + by) % 4) for i in range(4)]
            part = project(attended, (x + by) % 4).astype(jnp.bfloat16)
            got.append(lax.ppermute(part, ("side", "x"), pairs))
        return project(attended, x), got

    def along_zh(kept, got):
        partial = kept
        for g in got:
            partial = partial + g.astype(jnp.float32)
        low, high = partial[:, :wide], partial[:, wide:]
        give = jnp.where(zh == 0, high, low).astype(jnp.bfloat16)
        taken = lax.ppermute(give, ("side", "zh"), [(2, 3), (3, 2)])
        return (jnp.where(zh == 0, low, high) + taken.astype(jnp.float32)).astype(jnp.bfloat16)

    first_two = [exchange(blocks[j], flips[j]) for j in range(requests - 1)]
    attended = jnp.concatenate([serve(j, m) for j, m in enumerate(first_two)], axis=0)
    kept, got = along_x(attended)
    last = exchange(blocks[-1], flips[requests - 1])
    kept_last, got_last = along_x(serve(requests - 1, last))
    early = along_zh(kept, got)
    late = along_zh(kept_last, got_last)
    decoded = jnp.concatenate([early, late], axis=0)
    return jnp.where(side == 0, first, decoded)[None]


def solution(mesh):
    torus = Mesh(mesh.devices.reshape(mesh.shape["side"], 4, 4, 4, 2), AXES)
    in_specs = (
        P("side", ("y", "zl", "x", "zh"), None),
        P("side", ("y", "zl"), ("x", "zh")),
        P(),
        P(),
    )
    out_specs = P("side", ("y", "zl"), ("x", "zh"))
    return jax.shard_map(body, mesh=torus, in_specs=in_specs, out_specs=out_specs, check_vma=False)
```

```python
import jax
import jax.numpy as jnp
from jax import lax
from jax.experimental import pallas as pl
from jax.experimental.pallas import tpu as pltpu
from jax.sharding import Mesh
from jax.sharding import PartitionSpec as P


HEAD_DIM = 256
AXES = ("side", "y", "zl", "x", "zh")


def ring(value, axis, by):
    count = lax.axis_size(axis)
    return lax.ppermute(value, axis, [(i, (i + by) % count) for i in range(count)])


def ring_swap(value, bit):
    return lax.ppermute(value, "zl", [(i, i ^ bit) for i in range(4)])


def exchange(block, flip):
    groups = lax.axis_size("y") * lax.axis_size("zl")

    def route(by):
        pairs = [(p, groups + (p ^ by)) for p in range(groups)]
        return lambda b: lax.ppermute(b, ("side", "y", "zl"), pairs)

    return lax.switch(flip, [route(by) for by in range(groups)], block)


def attend_kernel(length_ref, queries_ref, memory_ref, out_ref):
    maxlen = memory_ref.shape[0]
    wide = out_ref.shape[1]
    shape = (queries_ref.shape[0], maxlen)
    valid = lax.broadcasted_iota(jnp.int32, shape, 1) < length_ref[0]
    scale = 1.0 / HEAD_DIM**0.5
    for e in range(wide // HEAD_DIM):
        cols = pl.ds(e * HEAD_DIM, HEAD_DIM)
        scores = lax.dot_general(
            queries_ref[:, cols],
            memory_ref[:, cols],
            (((1,), (1,)), ((), ())),
            preferred_element_type=jnp.float32,
        )
        scores = jnp.where(valid, scores * scale, -1e30)
        peak = jnp.max(scores, axis=-1, keepdims=True)
        expo = jnp.where(valid, jnp.exp(scores - peak), 0.0)
        total = jnp.sum(expo, axis=-1, keepdims=True)
        values = memory_ref[:, pl.ds(wide + e * HEAD_DIM, HEAD_DIM)]
        mixed = jnp.dot(expo.astype(jnp.bfloat16), values, preferred_element_type=jnp.float32)
        out_ref[:, cols] = (mixed / total).astype(jnp.bfloat16)


def attend(queries, memory, length):
    return pl.pallas_call(
        attend_kernel,
        out_shape=jax.ShapeDtypeStruct(queries.shape, jnp.bfloat16),
        in_specs=[
            pl.BlockSpec(memory_space=pltpu.SMEM),
            pl.BlockSpec(memory_space=pltpu.VMEM),
            pl.BlockSpec(memory_space=pltpu.VMEM),
        ],
        out_specs=pl.BlockSpec(memory_space=pltpu.VMEM),
    )(length, queries, memory)


def body(pool_rows, pool_weight, lengths, owner):
    side = lax.axis_index("side")
    y, zl, x, zh = (lax.axis_index(a) for a in AXES[1:])
    ny = lax.axis_size("y")
    requests = lengths.shape[1]
    w = pool_weight[0]
    mine = pool_rows[0]
    depth, width = w.shape
    wide = width // 2
    half = depth // 2
    count, model = mine.shape

    def both(value, axis):
        return ring(value, axis, 1), ring(value, axis, -1)

    def further(pair):
        return ring(pair[0][:half], "y", 1), ring(pair[1][half:], "y", -1)

    y0 = both(w, "y")
    u1 = ring_swap(w, 1)
    u2 = ring_swap(w, 2)
    x0 = both(mine, "x") + (ring(mine, "x", 2),)
    f0 = further(y0)
    y1 = both(u1, "y")
    u3 = ring_swap(u2, 1)
    y2 = both(u2, "y")
    other = lax.ppermute(mine, "zh", [(0, 1), (1, 0)])
    f1 = further(y1)
    y3 = both(u3, "y")
    x1 = both(other, "x") + (ring(other, "x", 2),)
    f2 = further(y2)
    f3 = further(y3)

    rows = jnp.zeros((8 * count, model), jnp.bfloat16)
    for parts, at in (((mine,) + x0, zh), ((other,) + x1, 1 - zh)):
        for part, place in zip(parts, (x, (x - 1) % 4, (x + 1) % 4, (x + 2) % 4)):
            rows = lax.dynamic_update_slice(rows, part, ((2 * place + at) * count, 0))
    mem_g = rows.shape[0]
    q_req = mem_g // requests
    maxlen = mem_g // 2

    acc = jnp.zeros((mem_g, width), jnp.float32)
    tail = jnp.zeros((wide, ny * 4 * depth), jnp.bfloat16)
    places = [y, (y - 1) % ny, (y + 1) % ny, (y + 2) % ny]
    for k, (u, p, f) in enumerate(((w, y0, f0), (u1, y1, f1), (u2, y2, f2), (u3, y3, f3))):
        block = jnp.concatenate((u,) + p + f, axis=0)
        starts = [(place * 4 + (zl ^ k)) * depth for place in places]
        cols = jnp.concatenate(
            [lax.dynamic_slice(rows, (0, at), (mem_g, depth)) for at in starts], axis=1
        )
        acc = acc + jnp.dot(cols, block, preferred_element_type=jnp.float32)
        turned = block[:, wide:].T
        for i, at in enumerate(starts):
            tail = lax.dynamic_update_slice(tail, turned[:, i * depth : (i + 1) * depth], (0, at))
    cached = acc.astype(jnp.bfloat16)
    first = cached[:, :wide]

    group = y * 4 + zl
    flips = owner[0]
    own = lax.dynamic_index_in_dim(lengths, group, 0, keepdims=False)
    begins = jnp.cumsum(own) - own
    padded = jnp.concatenate([cached, jnp.zeros((maxlen, width), jnp.bfloat16)], axis=0)
    blocks = [lax.dynamic_slice(padded, (begins[j], 0), (maxlen, width)) for j in range(requests)]

    def serve(j, memory):
        length = lax.dynamic_slice(lengths, (group ^ flips[j], j), (1, 1))[0]
        return attend(first[j * q_req : (j + 1) * q_req], memory, length)

    def project(attended, to):
        weight = lax.dynamic_slice(tail, (0, to * (2 * wide)), (wide, 2 * wide))
        return jnp.dot(attended, weight, preferred_element_type=jnp.float32)

    def along_x(attended):
        got = []
        for by in (2, 1, 3):
            pairs = [(4 + i, 4 + (i + by) % 4) for i in range(4)]
            part = project(attended, (x + by) % 4).astype(jnp.bfloat16)
            got.append(lax.ppermute(part, ("side", "x"), pairs))
        return project(attended, x), got

    def along_zh(kept, got):
        partial = kept
        for g in got:
            partial = partial + g.astype(jnp.float32)
        low, high = partial[:, :wide], partial[:, wide:]
        give = jnp.where(zh == 0, high, low).astype(jnp.bfloat16)
        taken = lax.ppermute(give, ("side", "zh"), [(2, 3), (3, 2)])
        return (jnp.where(zh == 0, low, high) + taken.astype(jnp.float32)).astype(jnp.bfloat16)

    first_two = [exchange(blocks[j], flips[j]) for j in range(requests - 1)]
    attended = jnp.concatenate([serve(j, m) for j, m in enumerate(first_two)], axis=0)
    kept, got = along_x(attended)
    last = exchange(blocks[-1], flips[requests - 1])
    kept_last, got_last = along_x(serve(requests - 1, last))
    early = along_zh(kept, got)
    late = along_zh(kept_last, got_last)
    decoded = jnp.concatenate([early, late], axis=0)
    return jnp.where(side == 0, first, decoded)[None]


def solution(mesh):
    torus = Mesh(mesh.devices.reshape(mesh.shape["side"], 4, 4, 4, 2), AXES)
    in_specs = (
        P("side", ("y", "zl", "x", "zh"), None),
        P("side", ("y", "zl"), ("x", "zh")),
        P(),
        P(),
    )
    out_specs = P("side", ("y", "zl"), ("x", "zh"))
    return jax.shard_map(body, mesh=torus, in_specs=in_specs, out_specs=out_specs, check_vma=False)
```

```python
import jax
import jax.numpy as jnp
from jax import lax
from jax.experimental import pallas as pl
from jax.experimental.pallas import tpu as pltpu
from jax.sharding import Mesh
from jax.sharding import PartitionSpec as P


HEAD_DIM = 256
AXES = ("side", "y", "zl", "x", "zh")


def ring(value, axis, by):
    count = lax.axis_size(axis)
    return lax.ppermute(value, axis, [(i, (i + by) % count) for i in range(count)])


def ring_swap(value, bit):
    return lax.ppermute(value, "zl", [(i, i ^ bit) for i in range(4)])


def exchange(block, flip):
    groups = lax.axis_size("y") * lax.axis_size("zl")

    def route(by):
        pairs = [(p, groups + (p ^ by)) for p in range(groups)]
        return lambda b: lax.ppermute(b, ("side", "y", "zl"), pairs)

    return lax.switch(flip, [route(by) for by in range(groups)], block)


def turn(pos_ref, depth):
    y, zl = pos_ref[2], pos_ref[3]
    places = [y, (y + 3) & 3, (y + 1) & 3, (y + 2) & 3]
    return lambda k, d: pl.multiple_of((places[d] * 4 + (zl ^ k)) * depth, depth)


def blocks_of(refs):
    u, p, m, a, b = refs
    return [u[...], p[...], m[...], jnp.concatenate([a[...], b[...]], axis=0)]


def near_kernel(pos_ref, *refs):
    parts, near, (rows_ref, acc_ref) = refs[:8], refs[8:18], refs[18:]
    count = parts[0].shape[0]
    x, zh = pos_ref[0], pos_ref[1]
    places = [x, (x + 3) & 3, (x + 1) & 3, (x + 2) & 3]
    for i, part in enumerate(parts):
        which = zh if i < 4 else 1 - zh
        at = pl.multiple_of((2 * places[i % 4] + which) * count, 16)
        rows_ref[pl.ds(at, count), :] = part[...]
    at = turn(pos_ref, near[0].shape[0])
    for k in range(2):
        for d, block in enumerate(blocks_of(near[5 * k : 5 * k + 5])):
            cols = rows_ref[:, pl.ds(at(k, d), block.shape[0])]
            new = jnp.dot(cols, block, preferred_element_type=jnp.float32)
            if k == 0 and d == 0:
                acc_ref[...] = new
            else:
                acc_ref[...] += new


def far_kernel(pos_ref, rows_ref, sum_ref, *refs):
    far, (out_ref, acc_ref) = refs[:10], refs[10:]
    at = turn(pos_ref, far[0].shape[0])
    for k in range(2):
        for d, block in enumerate(blocks_of(far[5 * k : 5 * k + 5])):
            cols = rows_ref[:, pl.ds(at(k + 2, d), block.shape[0])]
            new = jnp.dot(cols, block, preferred_element_type=jnp.float32)
            if k == 0 and d == 0:
                acc_ref[...] = sum_ref[...] + new
            else:
                acc_ref[...] += new
    out_ref[...] = acc_ref[...].astype(jnp.bfloat16)


def spread_kernel(pos_ref, attended_ref, *refs):
    held, out_ref = refs[:20], refs[20]
    x, y, zl = pos_ref[0], pos_ref[2], pos_ref[3]
    wide = attended_ref.shape[1]
    steps = [(y - x) & 3, (y - x + 3) & 3, (y - x + 1) & 3, (y - x + 2) & 3]
    attended = attended_ref[...]
    for k in range(4):
        u, p, m, a, b = held[5 * k : 5 * k + 5]
        tails = [r[:, pl.ds(wide, wide)] for r in (u, p, m, a, b)]
        tails = tails[:3] + [jnp.concatenate(tails[3:], axis=0)]
        depth = u.shape[0]
        at = pl.multiple_of((zl ^ k) * depth, depth)
        for d in range(4):
            new = lax.dot_general(
                attended, tails[d], (((1,), (1,)), ((), ())), preferred_element_type=jnp.float32
            )
            out_ref[steps[d], :, pl.ds(at, depth)] = new.astype(jnp.bfloat16)


INSIDE = pl.BlockSpec(memory_space=pltpu.VMEM)


def inside_call(kernel, scalars, operands, outs, scratch=(), limit=40):
    many = isinstance(outs, (list, tuple))
    return pl.pallas_call(
        kernel,
        out_shape=outs,
        in_specs=[pl.BlockSpec(memory_space=pltpu.SMEM)] + [INSIDE] * len(operands),
        out_specs=[INSIDE] * len(outs) if many else INSIDE,
        scratch_shapes=list(scratch),
        compiler_params=pltpu.CompilerParams(vmem_limit_bytes=limit * 2**20),
    )(scalars, *operands)


def attend_kernel(lengths_ref, queries_ref, *refs):
    memories, out_ref = refs[:-1], refs[-1]
    wide = out_ref.shape[1]
    rows = out_ref.shape[0] // len(memories)
    scale = 1.0 / HEAD_DIM**0.5
    for j, memory_ref in enumerate(memories):
        mine = pl.ds(j * rows, rows)
        shape = (rows, memory_ref.shape[0])
        valid = lax.broadcasted_iota(jnp.int32, shape, 1) < lengths_ref[j]
        for e in range(wide // HEAD_DIM):
            cols = pl.ds(e * HEAD_DIM, HEAD_DIM)
            scores = lax.dot_general(
                queries_ref[mine, cols],
                memory_ref[:, cols],
                (((1,), (1,)), ((), ())),
                preferred_element_type=jnp.float32,
            )
            scores = jnp.where(valid, scores * scale, -1e30)
            peak = jnp.max(scores, axis=-1, keepdims=True)
            expo = jnp.where(valid, jnp.exp(scores - peak), 0.0)
            total = jnp.sum(expo, axis=-1, keepdims=True)
            values = memory_ref[:, pl.ds(wide + e * HEAD_DIM, HEAD_DIM)]
            mixed = jnp.dot(expo.astype(jnp.bfloat16), values, preferred_element_type=jnp.float32)
            out_ref[mine, cols] = (mixed / total).astype(jnp.bfloat16)


def attend(queries, memories, lengths):
    out = jax.ShapeDtypeStruct(queries.shape, jnp.bfloat16)
    return inside_call(attend_kernel, lengths, [queries, *memories], out, limit=12)


def body(pool_rows, pool_weight, lengths, owner):
    side = lax.axis_index("side")
    y, zl, x, zh = (lax.axis_index(a) for a in AXES[1:])
    requests = lengths.shape[1]
    w = pool_weight[0]
    mine = pool_rows[0]
    depth, width = w.shape
    wide = width // 2
    half = depth // 2
    count, model = mine.shape

    def both(value, axis):
        return ring(value, axis, 1), ring(value, axis, -1)

    def further(pair):
        return ring(pair[0][:half], "y", 1), ring(pair[1][half:], "y", -1)

    y0 = both(w, "y")
    u1 = ring_swap(w, 1)
    u2 = ring_swap(w, 2)
    x0 = both(mine, "x") + (ring(mine, "x", 2),)
    f0 = further(y0)
    y1 = both(u1, "y")
    u3 = ring_swap(u2, 1)
    other = lax.ppermute(mine, "zh", [(0, 1), (1, 0)])
    y2 = both(u2, "y")
    f1 = further(y1)
    y3 = both(u3, "y")
    f2 = further(y2)
    x1 = both(other, "x") + (ring(other, "x", 2),)
    f3 = further(y3)

    mem_g = 8 * count
    maxlen = mem_g // 2
    pos = jnp.stack([x, zh, y, zl]).astype(jnp.int32)
    held = [(w, *y0, *f0), (u1, *y1, *f1), (u2, *y2, *f2), (u3, *y3, *f3)]
    sums = jax.ShapeDtypeStruct((mem_g, width), jnp.float32)
    rows, acc = inside_call(
        near_kernel,
        pos,
        [mine, *x0, other, *x1, *held[0], *held[1]],
        [jax.ShapeDtypeStruct((mem_g, model), jnp.bfloat16), sums],
    )
    cached = inside_call(
        far_kernel,
        pos,
        [rows, acc, *held[2], *held[3]],
        jax.ShapeDtypeStruct((mem_g, width), jnp.bfloat16),
        scratch=[pltpu.VMEM((mem_g, width), jnp.float32)],
    )
    first = cached[:, :wide]

    group = y * 4 + zl
    flips = owner[0]
    own = lax.dynamic_index_in_dim(lengths, group, 0, keepdims=False)
    begins = jnp.cumsum(own) - own
    served = jnp.concatenate(
        [lax.dynamic_slice(lengths, (group ^ flips[j], j), (1, 1))[0] for j in range(requests)]
    )
    begins = [begins[j] for j in range(requests)]
    padded = jnp.concatenate([cached, jnp.zeros((maxlen, width), jnp.bfloat16)], axis=0)
    blocks = [lax.dynamic_slice(padded, (begins[j], 0), (maxlen, width)) for j in range(requests)]
    memories = [exchange(blocks[j], flips[j]) for j in range(requests)]
    attended = attend(first, memories, served)

    parts = inside_call(
        spread_kernel,
        pos,
        [attended, *held[0], *held[1], *held[2], *held[3]],
        jax.ShapeDtypeStruct((4, mem_g, width), jnp.bfloat16),
    )
    got = []
    for by in (2, 1, 3):
        pairs = [(4 + i, 4 + (i + by) % 4) for i in range(4)]
        got.append(lax.ppermute(parts[by], ("side", "x"), pairs))
    partial = parts[0].astype(jnp.float32)
    for g in got:
        partial = partial + g.astype(jnp.float32)
    low, high = partial[:, :wide], partial[:, wide:]
    give = jnp.where(zh == 0, high, low).astype(jnp.bfloat16)
    taken = lax.ppermute(give, ("side", "zh"), [(2, 3), (3, 2)])
    decoded = (jnp.where(zh == 0, low, high) + taken.astype(jnp.float32)).astype(jnp.bfloat16)
    return jnp.where(side == 0, first, decoded)[None]


def solution(mesh):
    torus = Mesh(mesh.devices.reshape(mesh.shape["side"], 4, 4, 4, 2), AXES)
    in_specs = (
        P("side", ("y", "zl", "x", "zh"), None),
        P("side", ("y", "zl"), ("x", "zh")),
        P(),
        P(),
    )
    out_specs = P("side", ("y", "zl"), ("x", "zh"))
    return jax.shard_map(body, mesh=torus, in_specs=in_specs, out_specs=out_specs, check_vma=False)
```

```python
import jax
import jax.numpy as jnp
from jax import lax
from jax.experimental import pallas as pl
from jax.experimental.pallas import tpu as pltpu
from jax.sharding import Mesh
from jax.sharding import PartitionSpec as P


HEAD_DIM = 256
AXES = ("side", "y", "zl", "x", "zh")


def ring(value, axis, by):
    count = lax.axis_size(axis)
    return lax.ppermute(value, axis, [(i, (i + by) % count) for i in range(count)])


def ring_swap(value, bit):
    return lax.ppermute(value, "zl", [(i, i ^ bit) for i in range(4)])


def exchange(block, flip):
    groups = lax.axis_size("y") * lax.axis_size("zl")

    def route(by):
        pairs = [(p, groups + (p ^ by)) for p in range(groups)]
        return lambda b: lax.ppermute(b, ("side", "y", "zl"), pairs)

    return lax.switch(flip, [route(by) for by in range(groups)], block)


def turn(pos_ref, depth):
    y, zl = pos_ref[2], pos_ref[3]
    places = [y, (y + 3) & 3, (y + 1) & 3, (y + 2) & 3]
    return lambda k, d: pl.multiple_of((places[d] * 4 + (zl ^ k)) * depth, depth)


def fetch(held, buf_ref, sems):
    copies = []
    for k in range(2):
        u, p, m, a, b = held[5 * k : 5 * k + 5]
        half = a.shape[0]
        spots = [buf_ref.at[k, d] for d in range(3)]
        spots += [buf_ref.at[k, 3, pl.ds(0, half)], buf_ref.at[k, 3, pl.ds(half, half)]]
        for i, (src, dst) in enumerate(zip((u, p, m, a, b), spots)):
            copies.append(pltpu.make_async_copy(src, dst, sems.at[5 * k + i]))
    return copies


def accumulate(rows_ref, acc_ref, buf_ref, copies, at, base):
    depth = buf_ref.shape[2]
    for k in range(2):
        for d in range(4):
            for copy in copies[5 * k + d : 5 * k + d + (2 if d == 3 else 1)]:
                copy.wait()
            cols = rows_ref[:, pl.ds(at(k + base, d), depth)]
            new = jnp.dot(cols, buf_ref[k, d], preferred_element_type=jnp.float32)
            if base == 0 and k == 0 and d == 0:
                acc_ref[...] = new
            else:
                acc_ref[...] += new


def near_kernel(pos_ref, *refs):
    parts, near, (rows_ref, acc_ref, buf_ref, row_sems, sems) = refs[:8], refs[8:18], refs[18:]
    count = parts[0].shape[0]
    x, zh = pos_ref[0], pos_ref[1]
    places = [x, (x + 3) & 3, (x + 1) & 3, (x + 2) & 3]
    fills = []
    for i, part in enumerate(parts):
        which = zh if i < 4 else 1 - zh
        at = pl.multiple_of((2 * places[i % 4] + which) * count, 16)
        fills.append(pltpu.make_async_copy(part, rows_ref.at[pl.ds(at, count)], row_sems.at[i]))
    copies = fetch(near, buf_ref, sems)
    for copy in fills + copies:
        copy.start()
    for copy in fills:
        copy.wait()
    accumulate(rows_ref, acc_ref, buf_ref, copies, turn(pos_ref, buf_ref.shape[2]), 0)


def far_kernel(pos_ref, rows_ref, sum_ref, *refs):
    far, (out_ref, acc_ref, buf_ref, sems) = refs[:10], refs[10:]
    copies = fetch(far, buf_ref, sems)
    for copy in copies:
        copy.start()
    acc_ref[...] = sum_ref[...]
    accumulate(rows_ref, acc_ref, buf_ref, copies, turn(pos_ref, buf_ref.shape[2]), 2)
    out_ref[...] = acc_ref[...].astype(jnp.bfloat16)


def spread_kernel(pos_ref, attended_ref, *refs):
    held, outs, (buf_ref, sems) = refs[:20], refs[20:24], refs[24:]
    x, y, zl = pos_ref[0], pos_ref[2], pos_ref[3]
    wide = attended_ref.shape[1]
    steps = [(y - x) & 3, (y - x + 3) & 3, (y - x + 1) & 3, (y - x + 2) & 3]
    depth = held[0].shape[0]
    half = depth // 2
    tail = pl.ds(wide, wide)

    def start(src, i, at, rows):
        dst = buf_ref.at[i, pl.ds(at, rows)]
        pltpu.make_async_copy(src.at[:, tail], dst, sems.at[i]).start()

    for i, by in enumerate((2, 1, 3, 0)):
        for d in range(4):

            @pl.when(steps[d] == by)
            def _():
                for k in range(4):
                    at = pl.multiple_of((zl ^ k) * depth, depth)
                    if d < 3:
                        start(held[5 * k + d], i, at, depth)
                    else:
                        start(held[5 * k + 3], i, at, half)
                        start(held[5 * k + 4], i, pl.multiple_of(at + half, half), half)

    attended = attended_ref[...]
    for i, out_ref in enumerate(outs):
        pltpu.make_async_copy(buf_ref.at[i], buf_ref.at[i], sems.at[i]).wait()
        new = lax.dot_general(
            attended, buf_ref[i], (((1,), (1,)), ((), ())), preferred_element_type=jnp.float32
        )
        out_ref[...] = new.astype(out_ref.dtype)


def collect_kernel(pos_ref, own_ref, *refs):
    got, (keep_ref, give_ref, buf_ref, sems) = refs[:3], refs[3:]
    copies = [pltpu.make_async_copy(g, buf_ref.at[i], sems.at[i]) for i, g in enumerate(got)]
    for copy in copies:
        copy.start()
    total = own_ref[...]
    for i, copy in enumerate(copies):
        copy.wait()
        total = total + buf_ref[i].astype(jnp.float32)
    wide = keep_ref.shape[1]
    low, high = total[:, :wide], total[:, wide:]
    mine = pos_ref[1] == 0
    keep_ref[...] = jnp.where(mine, low, high)
    give_ref[...] = jnp.where(mine, high, low).astype(jnp.bfloat16)


INSIDE = pl.BlockSpec(memory_space=pltpu.VMEM)
ANYWHERE = pl.BlockSpec(memory_space=pltpu.HBM)


def call(kernel, scalars, inside, anywhere, outs, scratch=(), limit=40):
    many = isinstance(outs, (list, tuple))
    return pl.pallas_call(
        kernel,
        out_shape=outs,
        in_specs=[pl.BlockSpec(memory_space=pltpu.SMEM)]
        + [INSIDE] * len(inside)
        + [ANYWHERE] * len(anywhere),
        out_specs=[INSIDE] * len(outs) if many else INSIDE,
        scratch_shapes=list(scratch),
        compiler_params=pltpu.CompilerParams(vmem_limit_bytes=limit * 2**20),
    )(scalars, *inside, *anywhere)


def attend_kernel(lengths_ref, queries_ref, *refs):
    memories, out_ref = refs[:-1], refs[-1]
    wide = out_ref.shape[1]
    rows = out_ref.shape[0] // len(memories)
    scale = 1.0 / HEAD_DIM**0.5
    for j, memory_ref in enumerate(memories):
        mine = pl.ds(j * rows, rows)
        shape = (rows, memory_ref.shape[0])
        valid = lax.broadcasted_iota(jnp.int32, shape, 1) < lengths_ref[j]
        for e in range(wide // HEAD_DIM):
            cols = pl.ds(e * HEAD_DIM, HEAD_DIM)
            scores = lax.dot_general(
                queries_ref[mine, cols],
                memory_ref[:, cols],
                (((1,), (1,)), ((), ())),
                preferred_element_type=jnp.float32,
            )
            scores = jnp.where(valid, scores * scale, -1e30)
            peak = jnp.max(scores, axis=-1, keepdims=True)
            expo = jnp.where(valid, jnp.exp(scores - peak), 0.0)
            total = jnp.sum(expo, axis=-1, keepdims=True)
            values = memory_ref[:, pl.ds(wide + e * HEAD_DIM, HEAD_DIM)]
            mixed = jnp.dot(expo.astype(jnp.bfloat16), values, preferred_element_type=jnp.float32)
            out_ref[mine, cols] = (mixed / total).astype(jnp.bfloat16)


def attend(queries, memories, lengths):
    out = jax.ShapeDtypeStruct(queries.shape, jnp.bfloat16)
    return call(attend_kernel, lengths, [queries, *memories], [], out, limit=12)


def body(pool_rows, pool_weight, lengths, owner):
    side = lax.axis_index("side")
    y, zl, x, zh = (lax.axis_index(a) for a in AXES[1:])
    requests = lengths.shape[1]
    w = pool_weight[0]
    mine = pool_rows[0]
    depth, width = w.shape
    wide = width // 2
    half = depth // 2
    count, model = mine.shape

    def both(value, axis):
        return ring(value, axis, 1), ring(value, axis, -1)

    def further(pair):
        return ring(pair[0][:half], "y", 1), ring(pair[1][half:], "y", -1)

    y0 = both(w, "y")
    u1 = ring_swap(w, 1)
    u2 = ring_swap(w, 2)
    x0 = both(mine, "x") + (ring(mine, "x", 2),)
    f0 = further(y0)
    y1 = both(u1, "y")
    u3 = ring_swap(u2, 1)
    other = lax.ppermute(mine, "zh", [(0, 1), (1, 0)])
    y2 = both(u2, "y")
    f1 = further(y1)
    y3 = both(u3, "y")
    f2 = further(y2)
    x1 = both(other, "x") + (ring(other, "x", 2),)
    f3 = further(y3)

    mem_g = 8 * count
    maxlen = mem_g // 2
    pos = jnp.stack([x, zh, y, zl]).astype(jnp.int32)
    held = [(w, *y0, *f0), (u1, *y1, *f1), (u2, *y2, *f2), (u3, *y3, *f3)]
    sums = jax.ShapeDtypeStruct((mem_g, width), jnp.float32)
    buf = pltpu.VMEM((2, 4, depth, width), jnp.bfloat16)
    rows, acc = call(
        near_kernel,
        pos,
        [],
        [mine, *x0, other, *x1, *held[0], *held[1]],
        [jax.ShapeDtypeStruct((mem_g, model), jnp.bfloat16), sums],
        [buf, pltpu.SemaphoreType.DMA((8,)), pltpu.SemaphoreType.DMA((10,))],
        limit=60,
    )
    cached = call(
        far_kernel,
        pos,
        [rows, acc],
        [*held[2], *held[3]],
        jax.ShapeDtypeStruct((mem_g, width), jnp.bfloat16),
        [pltpu.VMEM((mem_g, width), jnp.float32), buf, pltpu.SemaphoreType.DMA((10,))],
        limit=60,
    )
    first = cached[:, :wide]

    group = y * 4 + zl
    flips = owner[0]
    own = lax.dynamic_index_in_dim(lengths, group, 0, keepdims=False)
    begins = jnp.cumsum(own) - own
    served = jnp.concatenate(
        [lax.dynamic_slice(lengths, (group ^ flips[j], j), (1, 1))[0] for j in range(requests)]
    )
    begins = [begins[j] for j in range(requests)]
    padded = jnp.concatenate([cached, jnp.zeros((maxlen, width), jnp.bfloat16)], axis=0)
    blocks = [lax.dynamic_slice(padded, (begins[j], 0), (maxlen, width)) for j in range(requests)]
    memories = [exchange(blocks[j], flips[j]) for j in range(requests)]
    attended = attend(first, memories, served)

    half_sum = jax.ShapeDtypeStruct((mem_g, width), jnp.bfloat16)
    *parts, own_part = call(
        spread_kernel,
        pos,
        [attended],
        [*held[0], *held[1], *held[2], *held[3]],
        [half_sum] * 3 + [sums],
        [pltpu.VMEM((4, 4 * depth, wide), jnp.bfloat16), pltpu.SemaphoreType.DMA((4,))],
        limit=60,
    )
    got = []
    for part, by in zip(parts, (2, 1, 3)):
        pairs = [(4 + i, 4 + (i + by) % 4) for i in range(4)]
        got.append(lax.ppermute(part, ("side", "x"), pairs))
    keep, give = call(
        collect_kernel,
        pos,
        [own_part],
        got,
        [
            jax.ShapeDtypeStruct((mem_g, wide), jnp.float32),
            jax.ShapeDtypeStruct((mem_g, wide), jnp.bfloat16),
        ],
        [pltpu.VMEM((3, mem_g, width), jnp.bfloat16), pltpu.SemaphoreType.DMA((3,))],
        limit=16,
    )
    taken = lax.ppermute(give, ("side", "zh"), [(2, 3), (3, 2)])
    decoded = (keep + taken.astype(jnp.float32)).astype(jnp.bfloat16)
    return jnp.where(side == 0, first, decoded)[None]


def solution(mesh):
    torus = Mesh(mesh.devices.reshape(mesh.shape["side"], 4, 4, 4, 2), AXES)
    in_specs = (
        P("side", ("y", "zl", "x", "zh"), None),
        P("side", ("y", "zl"), ("x", "zh")),
        P(),
        P(),
    )
    out_specs = P("side", ("y", "zl"), ("x", "zh"))
    return jax.shard_map(body, mesh=torus, in_specs=in_specs, out_specs=out_specs, check_vma=False)
```

```python
import jax
import jax.numpy as jnp
from jax import lax
from jax.experimental import pallas as pl
from jax.experimental.pallas import tpu as pltpu
from jax.sharding import Mesh
from jax.sharding import PartitionSpec as P


HEAD_DIM = 256
AXES = ("side", "y", "zl", "x", "zh")


def ring(value, axis, by):
    count = lax.axis_size(axis)
    return lax.ppermute(value, axis, [(i, (i + by) % count) for i in range(count)])


def ring_swap(value, bit):
    return lax.ppermute(value, "zl", [(i, i ^ bit) for i in range(4)])


def exchange(block, flip):
    groups = lax.axis_size("y") * lax.axis_size("zl")

    def route(by):
        pairs = [(p, groups + (p ^ by)) for p in range(groups)]
        return lambda b: lax.ppermute(b, ("side", "y", "zl"), pairs)

    return lax.switch(flip, [route(by) for by in range(groups)], block)


def turn(pos_ref, depth):
    y, zl = pos_ref[2], pos_ref[3]
    places = [y, (y + 3) & 3, (y + 1) & 3, (y + 2) & 3]
    return lambda k, d: pl.multiple_of((places[d] * 4 + (zl ^ k)) * depth, depth)


def fetch(held, buf_ref, sems):
    copies = []
    for k in range(2):
        u, p, m, a, b = held[5 * k : 5 * k + 5]
        half = a.shape[0]
        spots = [buf_ref.at[k, d] for d in range(3)]
        spots += [buf_ref.at[k, 3, pl.ds(0, half)], buf_ref.at[k, 3, pl.ds(half, half)]]
        for i, (src, dst) in enumerate(zip((u, p, m, a, b), spots)):
            copies.append(pltpu.make_async_copy(src, dst, sems.at[5 * k + i]))
    return copies


def accumulate(rows_ref, acc_ref, buf_ref, copies, at, base):
    depth = buf_ref.shape[2]
    for k in range(2):
        for d in range(4):
            for copy in copies[5 * k + d : 5 * k + d + (2 if d == 3 else 1)]:
                copy.wait()
            cols = rows_ref[:, pl.ds(at(k + base, d), depth)]
            new = jnp.dot(cols, buf_ref[k, d], preferred_element_type=jnp.float32)
            if base == 0 and k == 0 and d == 0:
                acc_ref[...] = new
            else:
                acc_ref[...] += new


def near_kernel(pos_ref, *refs):
    parts, near, (rows_ref, acc_ref, buf_ref, row_sems, sems) = refs[:8], refs[8:18], refs[18:]
    count = parts[0].shape[0]
    x, zh = pos_ref[0], pos_ref[1]
    places = [x, (x + 3) & 3, (x + 1) & 3, (x + 2) & 3]
    fills = []
    for i, part in enumerate(parts):
        which = zh if i < 4 else 1 - zh
        at = pl.multiple_of((2 * places[i % 4] + which) * count, 16)
        fills.append(pltpu.make_async_copy(part, rows_ref.at[pl.ds(at, count)], row_sems.at[i]))
    copies = fetch(near, buf_ref, sems)
    for copy in fills + copies:
        copy.start()
    for copy in fills:
        copy.wait()
    accumulate(rows_ref, acc_ref, buf_ref, copies, turn(pos_ref, buf_ref.shape[2]), 0)


def far_kernel(pos_ref, rows_ref, sum_ref, *refs):
    far, (out_ref, acc_ref, buf_ref, sems) = refs[:10], refs[10:]
    copies = fetch(far, buf_ref, sems)
    for copy in copies:
        copy.start()
    acc_ref[...] = sum_ref[...]
    accumulate(rows_ref, acc_ref, buf_ref, copies, turn(pos_ref, buf_ref.shape[2]), 2)
    out_ref[...] = acc_ref[...].astype(jnp.bfloat16)


def spread_kernel(pos_ref, attended_ref, *refs):
    held, outs, (buf_ref, sems) = refs[:20], refs[20:24], refs[24:]
    x, y, zl = pos_ref[0], pos_ref[2], pos_ref[3]
    wide = attended_ref.shape[1]
    steps = [(y - x) & 3, (y - x + 3) & 3, (y - x + 1) & 3, (y - x + 2) & 3]
    depth = held[0].shape[0]
    half = depth // 2
    tail = pl.ds(wide, wide)

    def start(src, i, at, rows):
        dst = buf_ref.at[i, pl.ds(at, rows)]
        pltpu.make_async_copy(src.at[:, tail], dst, sems.at[i]).start()

    for i, by in enumerate((2, 1, 3, 0)):
        for d in range(4):

            @pl.when(steps[d] == by)
            def _():
                for k in range(4):
                    at = pl.multiple_of((zl ^ k) * depth, depth)
                    if d < 3:
                        start(held[5 * k + d], i, at, depth)
                    else:
                        start(held[5 * k + 3], i, at, half)
                        start(held[5 * k + 4], i, pl.multiple_of(at + half, half), half)

    attended = attended_ref[...]
    for i, out_ref in enumerate(outs):
        pltpu.make_async_copy(buf_ref.at[i], buf_ref.at[i], sems.at[i]).wait()
        new = lax.dot_general(
            attended, buf_ref[i], (((1,), (1,)), ((), ())), preferred_element_type=jnp.float32
        )
        out_ref[...] = new.astype(out_ref.dtype)


def collect_kernel(pos_ref, own_ref, *refs):
    got, (keep_ref, give_ref, buf_ref, sems) = refs[:3], refs[3:]
    copies = [pltpu.make_async_copy(g, buf_ref.at[i], sems.at[i]) for i, g in enumerate(got)]
    for copy in copies:
        copy.start()
    total = own_ref[...]
    for i, copy in enumerate(copies):
        copy.wait()
        total = total + buf_ref[i].astype(jnp.float32)
    wide = keep_ref.shape[1]
    low, high = total[:, :wide], total[:, wide:]
    mine = pos_ref[1] == 0
    keep_ref[...] = jnp.where(mine, low, high)
    give_ref[...] = jnp.where(mine, high, low).astype(jnp.bfloat16)


INSIDE = pl.BlockSpec(memory_space=pltpu.VMEM)
ANYWHERE = pl.BlockSpec(memory_space=pltpu.HBM)


def call(kernel, scalars, inside, anywhere, outs, scratch=(), limit=40):
    many = isinstance(outs, (list, tuple))
    return pl.pallas_call(
        kernel,
        out_shape=outs,
        in_specs=[pl.BlockSpec(memory_space=pltpu.SMEM)]
        + [INSIDE] * len(inside)
        + [ANYWHERE] * len(anywhere),
        out_specs=[INSIDE] * len(outs) if many else INSIDE,
        scratch_shapes=list(scratch),
        compiler_params=pltpu.CompilerParams(vmem_limit_bytes=limit * 2**20),
    )(scalars, *inside, *anywhere)


def attend_kernel(lengths_ref, queries_ref, *refs):
    memories, out_ref = refs[:-1], refs[-1]
    wide = out_ref.shape[1]
    rows = out_ref.shape[0] // len(memories)
    scale = 1.0 / HEAD_DIM**0.5
    for j, memory_ref in enumerate(memories):
        mine = pl.ds(j * rows, rows)
        shape = (rows, memory_ref.shape[0])
        valid = lax.broadcasted_iota(jnp.int32, shape, 1) < lengths_ref[j]
        for e in range(wide // HEAD_DIM):
            cols = pl.ds(e * HEAD_DIM, HEAD_DIM)
            scores = lax.dot_general(
                queries_ref[mine, cols],
                memory_ref[:, cols],
                (((1,), (1,)), ((), ())),
                preferred_element_type=jnp.float32,
            )
            scores = jnp.where(valid, scores * scale, -1e30)
            peak = jnp.max(scores, axis=-1, keepdims=True)
            expo = jnp.where(valid, jnp.exp(scores - peak), 0.0)
            total = jnp.sum(expo, axis=-1, keepdims=True)
            values = memory_ref[:, pl.ds(wide + e * HEAD_DIM, HEAD_DIM)]
            mixed = jnp.dot(expo.astype(jnp.bfloat16), values, preferred_element_type=jnp.float32)
            out_ref[mine, cols] = (mixed / total).astype(jnp.bfloat16)


def attend(queries, memories, lengths):
    out = jax.ShapeDtypeStruct(queries.shape, jnp.bfloat16)
    return call(attend_kernel, lengths, [queries, *memories], [], out, limit=12)


def body(pool_rows, pool_weight, lengths, owner):
    side = lax.axis_index("side")
    y, zl, x, zh = (lax.axis_index(a) for a in AXES[1:])
    requests = lengths.shape[1]
    w = pool_weight[0]
    mine = pool_rows[0]
    depth, width = w.shape
    wide = width // 2
    half = depth // 2
    count, model = mine.shape

    def both(value, axis):
        return ring(value, axis, 1), ring(value, axis, -1)

    def further(pair):
        return ring(pair[0][:half], "y", 1), ring(pair[1][half:], "y", -1)

    y0 = both(w, "y")
    u1 = ring_swap(w, 1)
    u2 = ring_swap(w, 2)
    x0 = both(mine, "x") + (ring(mine, "x", 2),)
    f0 = further(y0)
    y1 = both(u1, "y")
    u3 = ring_swap(u2, 1)
    other = lax.ppermute(mine, "zh", [(0, 1), (1, 0)])
    y2 = both(u2, "y")
    f1 = further(y1)
    f2 = further(y2)
    x1 = both(other, "x") + (ring(other, "x", 2),)
    y3 = both(u3, "y")
    f3 = further(y3)

    mem_g = 8 * count
    maxlen = mem_g // 2
    pos = jnp.stack([x, zh, y, zl]).astype(jnp.int32)
    held = [(w, *y0, *f0), (u1, *y1, *f1), (u2, *y2, *f2), (u3, *y3, *f3)]
    sums = jax.ShapeDtypeStruct((mem_g, width), jnp.float32)
    buf = pltpu.VMEM((2, 4, depth, width), jnp.bfloat16)
    rows, acc = call(
        near_kernel,
        pos,
        [],
        [mine, *x0, other, *x1, *held[0], *held[1]],
        [jax.ShapeDtypeStruct((mem_g, model), jnp.bfloat16), sums],
        [buf, pltpu.SemaphoreType.DMA((8,)), pltpu.SemaphoreType.DMA((10,))],
        limit=60,
    )
    cached = call(
        far_kernel,
        pos,
        [rows, acc],
        [*held[2], *held[3]],
        jax.ShapeDtypeStruct((mem_g, width), jnp.bfloat16),
        [pltpu.VMEM((mem_g, width), jnp.float32), buf, pltpu.SemaphoreType.DMA((10,))],
        limit=52,
    )
    first = cached[:, :wide]

    group = y * 4 + zl
    flips = owner[0]
    own = lax.dynamic_index_in_dim(
        lengths, group, 0, keepdims=False, allow_negative_indices=False
    )
    begins = jnp.cumsum(own) - own
    served = jnp.concatenate(
        [lax.dynamic_slice(
            lengths, (group ^ flips[j], j), (1, 1), allow_negative_indices=False
        )[0]
            for j in range(requests)]
    )
    begins = [begins[j] for j in range(requests)]
    padded = jnp.concatenate([cached, jnp.zeros((maxlen, width), jnp.bfloat16)], axis=0)
    blocks = [lax.dynamic_slice(
        padded, (begins[j], 0), (maxlen, width), allow_negative_indices=False
    )
        for j in range(requests)]
    memories = [exchange(blocks[j], flips[j]) for j in range(requests)]
    attended = attend(first, memories, served)

    half_sum = jax.ShapeDtypeStruct((mem_g, width), jnp.bfloat16)
    *parts, own_part = call(
        spread_kernel,
        pos,
        [attended],
        [*held[0], *held[1], *held[2], *held[3]],
        [half_sum] * 3 + [sums],
        [pltpu.VMEM((4, 4 * depth, wide), jnp.bfloat16), pltpu.SemaphoreType.DMA((4,))],
        limit=60,
    )
    got = []
    for part, by in zip(parts, (2, 1, 3)):
        pairs = [(4 + i, 4 + (i + by) % 4) for i in range(4)]
        got.append(lax.ppermute(part, ("side", "x"), pairs))
    keep, give = call(
        collect_kernel,
        pos,
        [own_part],
        got,
        [
            jax.ShapeDtypeStruct((mem_g, wide), jnp.float32),
            jax.ShapeDtypeStruct((mem_g, wide), jnp.bfloat16),
        ],
        [pltpu.VMEM((3, mem_g, width), jnp.bfloat16), pltpu.SemaphoreType.DMA((3,))],
        limit=16,
    )
    taken = lax.ppermute(give, ("side", "zh"), [(2, 3), (3, 2)])
    decoded = (keep + taken.astype(jnp.float32)).astype(jnp.bfloat16)
    return jnp.where(side == 0, first, decoded)[None]


def solution(mesh):
    torus = Mesh(mesh.devices.reshape(mesh.shape["side"], 4, 4, 4, 2), AXES)
    in_specs = (
        P("side", ("y", "zl", "x", "zh"), None),
        P("side", ("y", "zl"), ("x", "zh")),
        P(),
        P(),
    )
    out_specs = P("side", ("y", "zl"), ("x", "zh"))
    return jax.shard_map(
        body, mesh=torus, in_specs=in_specs, out_specs=out_specs, check_vma=False
    )
```
